32 devices in a mesh: section: 4 (over y, core), rep: 2 (over x), tp: 4 (over z).
Axes of the slice: x: 2, y: 2, z: 4, core: 2. Of those that a mesh axis runs over, the one named last changes fastest.
Arguments:
- token_ids: int32 [2, 8, 128], P('rep', None, 'tp'), may hold values from 0 to 16383
- embed: bfloat16 [16384, 1024], P('section'), may hold values from -6 to 6
- w_in: bfloat16 [2, 4, 2, 1024, 2816], P('rep', 'section', None, None, 'tp'), may hold values from -0.1875 to 0.1875
- w_down: bfloat16 [2, 4, 2816, 1024], P('rep', 'section', 'tp'), may hold values from -0.109375 to 0.109375
- outer_in: float32 [4, 2, 1024, 2816], P('section', None, None, 'tp'), may hold values from -0.1875 to 0.1875
- outer_down: float32 [4, 2816, 1024], P('section', 'tp'), may hold values from -0.109375 to 0.109375
- moment_in: float32 [4, 2, 1024, 2816], P('section', None, None, 'tp'), may hold values from -0.12 to 0.12
- moment_down: float32 [4, 2816, 1024], P('section', 'tp'), may hold values from -0.12 to 0.12
- cotangent: bfloat16 [2, 8, 128, 1024], P('rep', None, 'tp'), may hold values from -6 to 6
- fragment: int32 [4], replicated, may hold values 0 or 1
Outputs:
- new_in: bfloat16 [2, 4, 2, 1024, 2816], P('rep', 'section', None, None, 'tp')
- new_down: bfloat16 [2, 4, 2816, 1024], P('rep', 'section', 'tp')
- next_outer_in: float32 [4, 2, 1024, 2816], P('section', None, None, 'tp')
- next_outer_down: float32 [4, 2816, 1024], P('section', 'tp')
- next_moment_in: float32 [4, 2, 1024, 2816], P('section', None, None, 'tp')
- next_moment_down: float32 [4, 2816, 1024], P('section', 'tp')
The draws below stay inside these ranges and needn't reach their ends.
All inputs are finite; a program needn't handle non-finite values.
Results may differ from the reference program's by a relative error of at most 0.03.
Values may be sent and summed in bfloat16 or wider, within the bound.
A program may use at most 128 MiB of HBM per device.

```python
import math
import jax
import jax.numpy as jnp
import numpy as np
from jax import lax

D = 1024
FF = 2816
VOCAB = 16384
MB = 8
MTOK = 128
LAYERS_SECTION = 1
LAYERS = 4
REPS = 2
N_SECTION = 4


def place_ends(drawn, own_key, low, high):
    dims = drawn.shape
    index_at = [jax.random.randint(jax.random.fold_in(own_key, axis), (), 0, dims[axis]) for axis in range(len(dims))]
    drawn = drawn.at[tuple(index_at)].set(low)
    longest = dims.index(max(dims))
    index_at[longest] = (index_at[longest] + 1) % dims[longest]
    return drawn.at[tuple(index_at)].set(high)


def steps_of(key, shape, shards, smallest, top_value):
    def one(dim, shards_of):
        draws = jax.random.uniform(jax.random.fold_in(jax.random.fold_in(key, 6), dim), (shards_of,), jnp.float32, smallest / len(shards), top_value / len(shards))
        return jnp.repeat(jnp.exp(draws), shape[dim] // shards_of).reshape((-1,) + (1,) * (len(shape) - dim - 1))

    loudness = one(*shards[0])
    for cut in shards[1:]:
        loudness = loudness * one(*cut)
    return loudness


def rank_bounds(number_of, slope):
    loads = [(1 << 20) // math.isqrt(rank ** slope) + 1 for rank in range(1, number_of + 1)]
    scale = 1 + sum(loads) // (1 << 30)
    return np.cumsum(np.array([max(1, weight // scale) for weight in loads]))


def ranked(rng, extent, count, slope):
    listing = rank_bounds(count, slope)
    ticket = jax.random.randint(jax.random.fold_in(rng, 1), extent, 0, int(listing[count - 1]))
    grade = jnp.searchsorted(jnp.asarray(listing, jnp.int32), ticket, side="right")
    return jax.random.permutation(jax.random.fold_in(rng, 2), count)[grade].astype(jnp.int32)


def noise(key, dims, scale, most, shards=(), kind=jnp.bfloat16):
    values = scale * jax.random.normal(key, dims, jnp.float32)
    if shards:
        values = values * steps_of(key, dims, shards, -0.22, 0.18)
    return jnp.clip(values, -most, most).astype(kind)


def setup_inputs(seed: int = 0) -> dict:
    arg_keys = jax.random.split(jax.random.key(seed), 11)
    return {
        "token_ids": place_ends(ranked(arg_keys[0], (REPS, MB, MTOK), VOCAB, 2), jax.random.fold_in(arg_keys[0], 3), 0, VOCAB - 1).astype(jnp.int32),
        "embed": noise(arg_keys[1], (VOCAB, D), 1.0, 6.0, ((0, 4),)),
        "w_in": noise(arg_keys[2], (REPS, LAYERS, 2, D, FF), D ** -0.5, 0.1875, ((0, 2), (1, 4), (4, 4))),
        "w_down": noise(arg_keys[3], (REPS, LAYERS, FF, D), FF ** -0.5, 0.109375, ((0, 2), (1, 4), (2, 4))),
        "outer_in": noise(arg_keys[4], (LAYERS, 2, D, FF), D ** -0.5, 0.1875, ((0, 4), (3, 4)), jnp.float32),
        "outer_down": noise(arg_keys[5], (LAYERS, FF, D), FF ** -0.5, 0.109375, ((0, 4), (1, 4)), jnp.float32),
        "moment_in": noise(arg_keys[6], (LAYERS, 2, D, FF), 0.02, 0.12, ((0, 4), (3, 4)), jnp.float32),
        "moment_down": noise(arg_keys[7], (LAYERS, FF, D), 0.02, 0.12, ((0, 4), (1, 4)), jnp.float32),
        "cotangent": noise(arg_keys[8], (REPS, MB, MTOK, D), 1.0, 6.0, ((0, 2), (2, 4))),
        "fragment": place_ends((jax.random.randint(arg_keys[9], (N_SECTION,), 0, 2) < 1).astype(jnp.int32), jax.random.fold_in(arg_keys[9], 1), 0, 1),
    }


EPS = 1e-05
INNER_LR = 0.001
OUTER_LR = 0.7
MOMENTUM = 0.9

def scale_rows(values):
    return lax.rsqrt(lax.optimization_barrier(jnp.mean(values * values, axis=-1, keepdims=True)) + EPS)

def layer_forward(x, pair, down):
    xf = x.astype(jnp.float32)
    rinv = scale_rows(xf)
    normed = (xf * rinv).astype(jnp.bfloat16)
    gate = jnp.dot(normed, pair[0], preferred_element_type=jnp.float32)
    upper = jnp.dot(normed, pair[1], preferred_element_type=jnp.float32)
    hidden = (jax.nn.silu(gate) * upper).astype(jnp.bfloat16)
    out = jnp.dot(hidden, down, preferred_element_type=jnp.float32)
    return ((xf + out).astype(jnp.bfloat16), (normed, gate, upper, hidden))

def layer_backward(grad, x, pair, down, saved):
    normed, gate, upper, hidden = saved
    d_hidden = jnp.dot(grad, down.T, preferred_element_type=jnp.float32)
    sig = jax.nn.sigmoid(gate)
    d_gate = (d_hidden * upper * sig * (1.0 + gate * (1.0 - sig))).astype(jnp.bfloat16)
    d_upper = (d_hidden * jax.nn.silu(gate)).astype(jnp.bfloat16)
    g_down = jnp.dot(hidden.T, grad, preferred_element_type=jnp.float32)
    g_pair = jnp.stack([jnp.dot(normed.T, d_gate, preferred_element_type=jnp.float32), jnp.dot(normed.T, d_upper, preferred_element_type=jnp.float32)])
    d_norm = jnp.dot(d_gate, pair[0].T, preferred_element_type=jnp.float32) + jnp.dot(d_upper, pair[1].T, preferred_element_type=jnp.float32)
    xf = x.astype(jnp.float32)
    rinv = scale_rows(xf)
    d_x = grad.astype(jnp.float32) + rinv * d_norm - xf * (rinv * rinv * rinv) * lax.optimization_barrier(jnp.mean(d_norm * xf, axis=-1, keepdims=True))
    return (d_x.astype(jnp.bfloat16), g_pair, g_down)

def reference(token_ids, embed, w_in, w_down, outer_in, outer_down, moment_in, moment_down, cotangent, fragment):
    chosen = fragment[jnp.arange(LAYERS) // LAYERS_SECTION] == 1
    inner_in = []
    inner_down = []
    for replica in range(REPS):
        x = jnp.take(embed, token_ids[replica].reshape(-1), axis=0)
        inputs = []
        saves = []
        for layer in range(LAYERS):
            inputs.append(x)
            x, saved = layer_forward(x, w_in[replica, layer], w_down[replica, layer])
            saves.append(saved)
        grad = cotangent[replica].reshape(-1, D)
        pair_list = [None] * LAYERS
        down_list = [None] * LAYERS
        for layer in reversed(range(LAYERS)):
            grad, g_pair, g_down = layer_backward(grad, inputs[layer], w_in[replica, layer], w_down[replica, layer], saves[layer])
            pair_list[layer] = (w_in[replica, layer].astype(jnp.float32) - INNER_LR * g_pair).astype(jnp.bfloat16)
            down_list[layer] = (w_down[replica, layer].astype(jnp.float32) - INNER_LR * g_down).astype(jnp.bfloat16)
        inner_in.append(jnp.stack(pair_list))
        inner_down.append(jnp.stack(down_list))
    inner_in = jnp.stack(inner_in)
    inner_down = jnp.stack(inner_down)
    mean_in = lax.optimization_barrier(jnp.mean(outer_in[None] - inner_in.astype(jnp.float32), axis=0))
    mean_down = lax.optimization_barrier(jnp.mean(outer_down[None] - inner_down.astype(jnp.float32), axis=0))
    moment_next_in = MOMENTUM * moment_in + mean_in
    moment_next_down = MOMENTUM * moment_down + mean_down
    outer_next_in = outer_in - OUTER_LR * (mean_in + MOMENTUM * moment_next_in)
    outer_next_down = outer_down - OUTER_LR * (mean_down + MOMENTUM * moment_next_down)
    pick_in = chosen[:, None, None, None]
    pick_down = chosen[:, None, None]
    new_in = jnp.where(pick_in[None], outer_next_in.astype(jnp.bfloat16)[None], inner_in)
    new_down = jnp.where(pick_down[None], outer_next_down.astype(jnp.bfloat16)[None], inner_down)
    return (new_in, new_down, jnp.where(pick_in, outer_next_in, outer_in), jnp.where(pick_down, outer_next_down, outer_down), jnp.where(pick_in, moment_next_in, moment_in), jnp.where(pick_down, moment_next_down, moment_down))
```

```python
import functools

import jax
import jax.numpy as jnp
from jax import lax
from jax.experimental import pallas as pl
from jax.experimental.pallas import tpu as pltpu
from jax.sharding import PartitionSpec as P

EPS = 1e-05
INNER_LR = 0.001
OUTER_LR = 0.7
MOMENTUM = 0.9
MESH = pl.DeviceIdType.MESH
NT = (((1,), (1,)), ((), ()))


def scale_rows(values):
    return lax.rsqrt(jnp.mean(values * values, axis=-1, keepdims=True) + EPS)


def dot(left, right):
    return jnp.dot(left, right, preferred_element_type=jnp.float32)


def dot_nt(left, right):
    return lax.dot_general(left, right, NT, preferred_element_type=jnp.float32)


def relay(
    sections,
    peers,
    x0,
    seeds,
    pair,
    down,
    normed_out,
    hidden_out,
    d_gate_out,
    d_up_out,
    grad_out,
    x_full,
    grad_full,
    part,
    back_part,
    inbox,
    back_inbox,
    rows_out,
    back_rows_out,
    gate_store,
    up_store,
    x_recv,
    grad_recv,
    part_recv,
    back_recv,
    x_send,
    grad_send,
    part_send,
    back_send,
    x_first,
    grad_first,
):
    section = lax.axis_index("section")
    me = lax.axis_index("tp")
    batches, own, _ = x0.shape
    first = section == 0
    final = section == sections - 1
    later = section < sections - 1
    after = section > 0

    def rows_of(index):
        return pl.ds(pl.multiple_of(index * own, own), own)

    mine = rows_of(me)

    def wait(ref, sem):
        pltpu.make_async_copy(ref, ref, sem).wait()

    def send(source, target, send_sem, recv_sem, device):
        pltpu.make_async_remote_copy(
            src_ref=source,
            dst_ref=target,
            send_sem=send_sem,
            recv_sem=recv_sem,
            device_id=device,
            device_id_type=MESH,
        ).start()

    def around(offset):
        return lax.rem(me + offset, peers)

    barrier = pltpu.get_barrier_semaphore()
    for offset in range(1, peers):
        pl.semaphore_signal(
            barrier, inc=1, device_id={"tp": around(offset)}, device_id_type=MESH
        )

    @pl.when(later)
    def _():
        for offset in range(peers):
            pl.semaphore_signal(
                barrier,
                inc=1,
                device_id={"section": section + 1, "tp": around(offset)},
                device_id_type=MESH,
            )

    @pl.when(after)
    def _():
        for offset in range(peers):
            pl.semaphore_signal(
                barrier,
                inc=1,
                device_id={"section": section - 1, "tp": around(offset)},
                device_id_type=MESH,
            )

    @pl.when(later & after)
    def _():
        pl.semaphore_wait(barrier, 3 * peers - 1)

    @pl.when(jnp.logical_not(later & after))
    def _():
        pl.semaphore_wait(barrier, 2 * peers - 1)

    def feed(rows, full, send_sem, recv_sem):
        def step(micro, carry):
            for offset in range(1, peers):
                send(
                    rows.at[micro],
                    full.at[micro, mine],
                    send_sem.at[micro],
                    recv_sem.at[micro],
                    {"tp": around(offset)},
                )
            full[micro, mine, :] = rows[micro]
            return carry

        lax.fori_loop(0, batches, step, 0)

    @pl.when(first)
    def _():
        feed(x0, x_full, x_first, x_recv)

    @pl.when(final)
    def _():
        feed(seeds, grad_full, grad_first, grad_recv)

    def arrive(micro, full, recv_sem, alone):
        @pl.when(alone)
        def _():
            wait(full.at[micro, pl.ds(0, (peers - 1) * own)], recv_sem.at[micro])

        @pl.when(jnp.logical_not(alone))
        def _():
            wait(full.at[micro], recv_sem.at[micro])

    def scatter(micro, source, box, send_sem, recv_sem):
        for offset in range(1, peers):
            send(
                source.at[micro, rows_of(around(offset))],
                box.at[micro, offset - 1],
                send_sem.at[micro],
                recv_sem.at[micro],
                {"tp": around(offset)},
            )

    def collect(micro, source, box, recv_sem):
        wait(box.at[micro], recv_sem.at[micro])
        total = source[micro, mine, :].astype(jnp.float32)
        for slot in range(peers - 1):
            total += box[micro, slot].astype(jnp.float32)
        return total

    def pass_along(micro, rows, full, send_sem, recv_sem, step):
        for offset in range(peers):
            send(
                rows.at[micro],
                full.at[micro, mine],
                send_sem.at[micro],
                recv_sem.at[micro],
                {"section": section + step, "tp": around(offset)},
            )

    def forward(micro):
        arrive(micro, x_full, x_recv, first)
        xf = x_full[micro].astype(jnp.float32)
        normed = (xf * scale_rows(xf)).astype(jnp.bfloat16)
        normed_out[micro] = normed
        gate = dot(normed, pair[0])
        upper = dot(normed, pair[1])
        gate_store[micro] = gate
        up_store[micro] = upper
        hidden = (gate * jax.nn.sigmoid(gate) * upper).astype(jnp.bfloat16)
        hidden_out[micro] = hidden

        @pl.when(later)
        def _():
            part[micro] = dot(hidden, down[...]).astype(jnp.bfloat16)
            scatter(micro, part, inbox, part_send, part_recv)

    def forward_end(micro):
        total = collect(micro, part, inbox, part_recv)
        xf = x_full[micro, mine, :].astype(jnp.float32)
        rows_out[micro] = (xf + total).astype(jnp.bfloat16)
        pass_along(micro, rows_out, x_full, x_send, x_recv, 1)

    def backward(micro):
        arrive(micro, grad_full, grad_recv, final)
        grad = grad_full[micro]
        grad_out[micro] = grad
        d_hidden = dot_nt(grad, down[...])
        gate = gate_store[micro]
        sig = jax.nn.sigmoid(gate)
        d_gate = (d_hidden * up_store[micro] * sig * (1.0 + gate * (1.0 - sig))).astype(
            jnp.bfloat16
        )
        d_up = (d_hidden * (gate * sig)).astype(jnp.bfloat16)
        d_gate_out[micro] = d_gate
        d_up_out[micro] = d_up

        @pl.when(after)
        def _():
            back_part[micro] = (dot_nt(d_gate, pair[0]) + dot_nt(d_up, pair[1])).astype(
                jnp.bfloat16
            )
            scatter(micro, back_part, back_inbox, back_send, back_recv)

    def backward_end(micro):
        d_norm = collect(micro, back_part, back_inbox, back_recv)
        xf = x_full[micro, mine, :].astype(jnp.float32)
        rinv = scale_rows(xf)
        d_x = (
            grad_full[micro, mine, :].astype(jnp.float32)
            + rinv * d_norm
            - xf * (rinv * rinv * rinv) * jnp.mean(d_norm * xf, axis=-1, keepdims=True)
        )
        back_rows_out[micro] = d_x.astype(jnp.bfloat16)
        pass_along(micro, back_rows_out, grad_full, grad_send, grad_recv, -1)

    delay = 2 * (sections - 1 - section)

    def step(tick, carry):
        @pl.when(tick < batches)
        def _():
            forward(tick)

        @pl.when(later & (tick >= 1) & (tick <= batches))
        def _():
            forward_end(tick - 1)

        micro = tick - delay

        @pl.when((micro >= 0) & (micro < batches))
        def _():
            backward(micro)

        @pl.when(after & (micro >= 1) & (micro <= batches))
        def _():
            backward_end(micro - 1)

        return carry

    lax.fori_loop(0, batches + 2 * (sections - 1) + 1, step, 0)

    def drain(micro, carry):
        some = pl.ds(0, (peers - 1) * own)

        @pl.when(first)
        def _():
            wait(x_full.at[micro, some], x_first.at[micro])

        @pl.when(final)
        def _():
            wait(grad_full.at[micro, some], grad_first.at[micro])

        @pl.when(later)
        def _():
            wait(part.at[micro, some], part_send.at[micro])
            wait(x_full.at[micro], x_send.at[micro])

        @pl.when(after)
        def _():
            wait(back_part.at[micro, some], back_send.at[micro])
            wait(grad_full.at[micro], grad_send.at[micro])

        return carry

    lax.fori_loop(0, batches, drain, 0)


def run_relay(x0, seeds, pair, down):
    sections, peers = lax.axis_size("section"), lax.axis_size("tp")
    batches, own, width = x0.shape
    hidden = down.shape[0]
    rows = own * peers

    def of(*shape, kind=jnp.bfloat16):
        return pltpu.VMEM((batches,) + shape, kind)

    def out(columns):
        return jax.ShapeDtypeStruct((batches, rows, columns), jnp.bfloat16)

    vmem = pl.BlockSpec(memory_space=pltpu.VMEM)
    flops = 2 * batches * rows * width * hidden * 6
    return pl.pallas_call(
        functools.partial(relay, sections, peers),
        out_shape=(out(width), out(hidden), out(hidden), out(hidden), out(width)),
        in_specs=[vmem] * 4,
        out_specs=(vmem,) * 5,
        scratch_shapes=[
            of(rows, width),
            of(rows, width),
            of(rows, width),
            of(rows, width),
            of(peers - 1, own, width),
            of(peers - 1, own, width),
            of(own, width),
            of(own, width),
            of(rows, hidden, kind=jnp.float32),
            of(rows, hidden, kind=jnp.float32),
        ]
        + [pltpu.SemaphoreType.DMA((batches,))] * 10,
        compiler_params=pltpu.CompilerParams(
            collective_id=0, has_side_effects=True, vmem_limit_bytes=60 * 1024 * 1024
        ),
        cost_estimate=pl.CostEstimate(
            flops=flops, bytes_accessed=32 * 1024 * 1024, transcendentals=0
        ),
    )(x0, seeds, pair, down)


def shards(
    token_ids,
    embed,
    w_in,
    w_down,
    outer_in,
    outer_down,
    moment_in,
    moment_down,
    cotangent,
    fragment,
):
    sections = lax.axis_size("section")
    section = lax.axis_index("section")
    replicas = lax.axis_size("rep")
    ids = token_ids[0]
    batches, own_rows = ids.shape
    vocab_part, width = embed.shape
    local_ids = ids - section * vocab_part
    inside = (local_ids >= 0) & (local_ids < vocab_part)
    looked = jnp.take(embed, jnp.clip(local_ids, 0, vocab_part - 1), axis=0).astype(jnp.float32)
    looked = jnp.where(inside[:, :, None], looked, 0.0)
    start_rows = lax.psum(looked.astype(jnp.bfloat16), "section")
    pairs = w_in[0, 0]
    downs = w_down[0, 0]
    normed, hidden, d_gate, d_up, grad = run_relay(start_rows, cotangent[0], pairs, downs)

    def weight_grad(left, right):
        return jnp.einsum("bti,btj->ij", left, right, preferred_element_type=jnp.float32)

    def other(values):
        return lax.ppermute(
            values, "rep", [(source, (source + 1) % replicas) for source in range(replicas)]
        )

    def total(values):
        summed = values.astype(jnp.float32)
        passing = values
        for _ in range(replicas - 1):
            passing = other(passing)
            summed = summed + passing.astype(jnp.float32)
        return summed

    def inner(weights, grads):
        return (weights.astype(jnp.float32) - INNER_LR * grads).astype(jnp.bfloat16)

    flag = lax.dynamic_index_in_dim(fragment, section, 0, keepdims=False)
    chosen = flag == 1

    def update(weights, grads, outer, moment):
        new = inner(weights, grads)
        mean = outer - total(new) / replicas
        next_moment = MOMENTUM * moment + mean
        next_outer = outer - OUTER_LR * (mean + MOMENTUM * next_moment)
        return (
            jnp.where(chosen, next_outer.astype(jnp.bfloat16), new),
            jnp.where(chosen, next_outer, outer),
            jnp.where(chosen, next_moment, moment),
        )

    down_new, down_outer, down_moment = update(
        downs, weight_grad(hidden, grad), outer_down[0], moment_down[0]
    )
    gate_new, gate_outer, gate_moment = update(
        pairs[0], weight_grad(normed, d_gate), outer_in[0, 0], moment_in[0, 0]
    )
    up_new, up_outer, up_moment = update(
        pairs[1], weight_grad(normed, d_up), outer_in[0, 1], moment_in[0, 1]
    )
    return (
        jnp.stack([gate_new, up_new])[None, None],
        down_new[None, None],
        jnp.stack([gate_outer, up_outer])[None],
        down_outer[None],
        jnp.stack([gate_moment, up_moment])[None],
        down_moment[None],
    )


def solution(mesh):
    return jax.shard_map(
        shards,
        mesh=mesh,
        in_specs=(
            P("rep", None, "tp"),
            P("section", None),
            P("rep", "section", None, None, "tp"),
            P("rep", "section", "tp", None),
            P("section", None, None, "tp"),
            P("section", "tp", None),
            P("section", None, None, "tp"),
            P("section", "tp", None),
            P("rep", None, "tp", None),
            P(),
        ),
        out_specs=(
            P("rep", "section", None, None, "tp"),
            P("rep", "section", "tp", None),
            P("section", None, None, "tp"),
            P("section", "tp", None),
            P("section", None, None, "tp"),
            P("section", "tp", None),
        ),
        check_vma=False,
    )
```

```python
import functools

import jax
import jax.numpy as jnp
from jax import lax
from jax.experimental import pallas as pl
from jax.experimental.pallas import tpu as pltpu
from jax.sharding import PartitionSpec as P

EPS = 1e-05
INNER_LR = 0.001
OUTER_LR = 0.7
MOMENTUM = 0.9
DELAY = 4
MESH = pl.DeviceIdType.MESH
NT = (((1,), (1,)), ((), ()))


def scale_rows(values):
    return lax.rsqrt(jnp.mean(values * values, axis=-1, keepdims=True) + EPS)


def dot(left, right):
    return jnp.dot(left, right, preferred_element_type=jnp.float32)


def dot_nt(left, right):
    return lax.dot_general(left, right, NT, preferred_element_type=jnp.float32)


def relay(
    sections,
    peers,
    looked,
    seeds,
    pair,
    down,
    normed_out,
    hidden_out,
    d_gate_out,
    d_up_out,
    grad_out,
    x_full,
    grad_full,
    part,
    back_part,
    inbox,
    back_inbox,
    rows_out,
    back_rows_out,
    gate_store,
    up_store,
    x_recv,
    grad_recv,
    part_recv,
    back_recv,
    x_send,
    grad_send,
    part_send,
    back_send,
    x_first,
    grad_first,
    rows_in,
    looked_box,
    looked_recv,
    looked_send,
):
    section = lax.axis_index("section")
    me = lax.axis_index("tp")
    batches, own, _ = looked.shape
    first = section == 0
    final = section == sections - 1
    later = section < sections - 1
    after = section > 0

    def rows_of(index):
        return pl.ds(pl.multiple_of(index * own, own), own)

    mine = rows_of(me)

    def wait(ref, sem):
        pltpu.make_async_copy(ref, ref, sem).wait()

    def send(source, target, send_sem, recv_sem, device):
        pltpu.make_async_remote_copy(
            src_ref=source,
            dst_ref=target,
            send_sem=send_sem,
            recv_sem=recv_sem,
            device_id=device,
            device_id_type=MESH,
        ).start()

    def around(offset):
        return lax.rem(me + offset, peers)

    barrier = pltpu.get_barrier_semaphore()
    for offset in range(1, peers):
        pl.semaphore_signal(
            barrier, inc=1, device_id={"tp": around(offset)}, device_id_type=MESH
        )

    @pl.when(later)
    def _():
        for offset in range(peers):
            pl.semaphore_signal(
                barrier,
                inc=1,
                device_id={"section": section + 1, "tp": around(offset)},
                device_id_type=MESH,
            )

    @pl.when(after)
    def _():
        for offset in range(peers):
            pl.semaphore_signal(
                barrier,
                inc=1,
                device_id={"section": section - 1, "tp": around(offset)},
                device_id_type=MESH,
            )

    @pl.when(first)
    def _():
        for other in range(2, sections):
            pl.semaphore_signal(
                barrier, inc=1, device_id={"section": other}, device_id_type=MESH
            )
        pl.semaphore_wait(barrier, 2 * peers - 1 + max(sections - 2, 0))

    @pl.when(section == 1)
    def _():
        pl.semaphore_wait(barrier, (3 if sections > 2 else 2) * peers - 1)

    @pl.when(section >= 2)
    def _():
        pl.semaphore_signal(barrier, inc=1, device_id={"section": 0}, device_id_type=MESH)

    @pl.when((section >= 2) & later)
    def _():
        pl.semaphore_wait(barrier, 3 * peers)

    @pl.when((section >= 2) & final)
    def _():
        pl.semaphore_wait(barrier, 2 * peers)

    def spread(micro, rows, full, send_sem, recv_sem):
        for offset in range(1, peers):
            send(
                rows.at[micro],
                full.at[micro, mine],
                send_sem.at[micro],
                recv_sem.at[micro],
                {"tp": around(offset)},
            )
        full[micro, mine, :] = rows[micro]

    def feed(micro):
        total = looked[micro]
        for slot in range(sections - 1):
            wait(looked_box.at[slot, micro], looked_recv.at[slot, micro])
            total += looked_box[slot, micro]
        rows_in[micro] = total
        spread(micro, rows_in, x_full, x_first, x_recv)

    @pl.when(after)
    def _():
        def give(micro, carry):
            send(
                looked.at[micro],
                looked_box.at[section - 1, micro],
                looked_send.at[micro],
                looked_recv.at[section - 1, micro],
                {"section": 0},
            )
            return carry

        lax.fori_loop(0, batches, give, 0)

    @pl.when(final)
    def _():
        def give(micro, carry):
            spread(micro, seeds, grad_full, grad_first, grad_recv)
            return carry

        lax.fori_loop(0, batches, give, 0)

    @pl.when(first)
    def _():
        for micro in range(min(2, batches)):
            feed(micro)

    def arrive(micro, full, recv_sem, alone):
        @pl.when(alone)
        def _():
            wait(full.at[micro, pl.ds(0, (peers - 1) * own)], recv_sem.at[micro])

        @pl.when(jnp.logical_not(alone))
        def _():
            wait(full.at[micro], recv_sem.at[micro])

    def scatter(micro, source, box, send_sem, recv_sem):
        for offset in range(1, peers):
            send(
                source.at[micro, rows_of(around(offset))],
                box.at[micro, offset - 1],
                send_sem.at[micro],
                recv_sem.at[micro],
                {"tp": around(offset)},
            )

    def collect(micro, source, box, recv_sem):
        wait(box.at[micro], recv_sem.at[micro])
        total = source[micro, mine, :].astype(jnp.float32)
        for slot in range(peers - 1):
            total += box[micro, slot].astype(jnp.float32)
        return total

    def pass_along(micro, rows, full, send_sem, recv_sem, step):
        for offset in range(peers):
            send(
                rows.at[micro],
                full.at[micro, mine],
                send_sem.at[micro],
                recv_sem.at[micro],
                {"section": section + step, "tp": around(offset)},
            )

    def forward(micro):
        arrive(micro, x_full, x_recv, first)
        xf = x_full[micro].astype(jnp.float32)
        normed = (xf * scale_rows(xf)).astype(jnp.bfloat16)
        normed_out[micro] = normed
        gate = dot(normed, pair[0])
        upper = dot(normed, pair[1])
        gate_store[micro] = gate
        up_store[micro] = upper
        hidden = (gate * jax.nn.sigmoid(gate) * upper).astype(jnp.bfloat16)
        hidden_out[micro] = hidden

        @pl.when(later)
        def _():
            part[micro] = dot(hidden, down[...]).astype(jnp.bfloat16)
            scatter(micro, part, inbox, part_send, part_recv)

    def forward_end(micro):
        total = collect(micro, part, inbox, part_recv)
        xf = x_full[micro, mine, :].astype(jnp.float32)
        rows_out[micro] = (xf + total).astype(jnp.bfloat16)
        pass_along(micro, rows_out, x_full, x_send, x_recv, 1)

    def backward(micro):
        arrive(micro, grad_full, grad_recv, final)
        grad = grad_full[micro]
        grad_out[micro] = grad
        d_hidden = dot_nt(grad, down[...])
        gate = gate_store[micro]
        sig = jax.nn.sigmoid(gate)
        d_gate = (d_hidden * up_store[micro] * sig * (1.0 + gate * (1.0 - sig))).astype(
            jnp.bfloat16
        )
        d_up = (d_hidden * (gate * sig)).astype(jnp.bfloat16)
        d_gate_out[micro] = d_gate
        d_up_out[micro] = d_up

        @pl.when(after)
        def _():
            back_part[micro] = (dot_nt(d_gate, pair[0]) + dot_nt(d_up, pair[1])).astype(
                jnp.bfloat16
            )
            scatter(micro, back_part, back_inbox, back_send, back_recv)

    def backward_end(micro):
        d_norm = collect(micro, back_part, back_inbox, back_recv)
        xf = x_full[micro, mine, :].astype(jnp.float32)
        rinv = scale_rows(xf)
        d_x = (
            grad_full[micro, mine, :].astype(jnp.float32)
            + rinv * d_norm
            - xf * (rinv * rinv * rinv) * jnp.mean(d_norm * xf, axis=-1, keepdims=True)
        )
        back_rows_out[micro] = d_x.astype(jnp.bfloat16)
        pass_along(micro, back_rows_out, grad_full, grad_send, grad_recv, -1)

    delay = DELAY * (sections - 1 - section)

    def step(tick, carry):
        @pl.when(first & (tick + 2 < batches))
        def _():
            feed(tick + 2)

        @pl.when(tick < batches)
        def _():
            forward(tick)

        @pl.when(later & (tick >= 1) & (tick <= batches))
        def _():
            forward_end(tick - 1)

        micro = tick - delay

        @pl.when((micro >= 0) & (micro < batches))
        def _():
            backward(micro)

        @pl.when(after & (micro >= 1) & (micro <= batches))
        def _():
            backward_end(micro - 1)

        return carry

    lax.fori_loop(0, batches + DELAY * (sections - 1) + 1, step, 0)

    def drain(micro, carry):
        some = pl.ds(0, (peers - 1) * own)

        @pl.when(first)
        def _():
            wait(x_full.at[micro, some], x_first.at[micro])

        @pl.when(final)
        def _():
            wait(grad_full.at[micro, some], grad_first.at[micro])

        @pl.when(later)
        def _():
            wait(part.at[micro, some], part_send.at[micro])
            wait(x_full.at[micro], x_send.at[micro])

        @pl.when(after)
        def _():
            wait(looked.at[micro], looked_send.at[micro])
            wait(back_part.at[micro, some], back_send.at[micro])
            wait(grad_full.at[micro], grad_send.at[micro])

        return carry

    lax.fori_loop(0, batches, drain, 0)


def run_relay(x0, seeds, pair, down):
    sections, peers = lax.axis_size("section"), lax.axis_size("tp")
    batches, own, width = x0.shape
    hidden = down.shape[0]
    rows = own * peers

    def of(*shape, kind=jnp.bfloat16):
        return pltpu.VMEM((batches,) + shape, kind)

    def out(columns):
        return jax.ShapeDtypeStruct((batches, rows, columns), jnp.bfloat16)

    vmem = pl.BlockSpec(memory_space=pltpu.VMEM)
    flops = 2 * batches * rows * width * hidden * 6
    return pl.pallas_call(
        functools.partial(relay, sections, peers),
        out_shape=(out(width), out(hidden), out(hidden), out(hidden), out(width)),
        in_specs=[vmem] * 4,
        out_specs=(vmem,) * 5,
        scratch_shapes=[
            of(rows, width),
            of(rows, width),
            of(rows, width),
            of(rows, width),
            of(peers - 1, own, width),
            of(peers - 1, own, width),
            of(own, width),
            of(own, width),
            of(rows, hidden, kind=jnp.float32),
            of(rows, hidden, kind=jnp.float32),
        ]
        + [pltpu.SemaphoreType.DMA((batches,))] * 10
        + [
            of(own, width),
            pltpu.VMEM((sections - 1, batches, own, width), jnp.bfloat16),
            pltpu.SemaphoreType.DMA((sections - 1, batches)),
            pltpu.SemaphoreType.DMA((batches,)),
        ],
        compiler_params=pltpu.CompilerParams(
            collective_id=0, has_side_effects=True, vmem_limit_bytes=60 * 1024 * 1024
        ),
        cost_estimate=pl.CostEstimate(
            flops=flops, bytes_accessed=32 * 1024 * 1024, transcendentals=0
        ),
    )(x0, seeds, pair, down)


def shards(
    token_ids,
    embed,
    w_in,
    w_down,
    outer_in,
    outer_down,
    moment_in,
    moment_down,
    cotangent,
    fragment,
):
    sections = lax.axis_size("section")
    section = lax.axis_index("section")
    replicas = lax.axis_size("rep")
    ids = token_ids[0]
    batches, own_rows = ids.shape
    vocab_part, width = embed.shape
    local_ids = ids - section * vocab_part
    inside = (local_ids >= 0) & (local_ids < vocab_part)
    looked = jnp.take(embed, jnp.clip(local_ids, 0, vocab_part - 1), axis=0)
    start_rows = jnp.where(inside[:, :, None], looked, jnp.zeros_like(looked))
    pairs = w_in[0, 0]
    downs = w_down[0, 0]
    normed, hidden, d_gate, d_up, grad = run_relay(start_rows, cotangent[0], pairs, downs)

    def weight_grad(left, right):
        return jnp.einsum("bti,btj->ij", left, right, preferred_element_type=jnp.float32)

    def other(values):
        return lax.ppermute(
            values, "rep", [(source, (source + 1) % replicas) for source in range(replicas)]
        )

    def total(values):
        summed = values.astype(jnp.float32)
        passing = values
        for _ in range(replicas - 1):
            passing = other(passing)
            summed = summed + passing.astype(jnp.float32)
        return summed

    def inner(weights, grads):
        return (weights.astype(jnp.float32) - INNER_LR * grads).astype(jnp.bfloat16)

    flag = lax.dynamic_index_in_dim(fragment, section, 0, keepdims=False)
    chosen = flag == 1

    new = (
        inner(downs, weight_grad(hidden, grad)),
        inner(pairs[0], weight_grad(normed, d_gate)),
        inner(pairs[1], weight_grad(normed, d_up)),
    )
    outers = (outer_down[0], outer_in[0, 0], outer_in[0, 1])
    moments = (moment_down[0], moment_in[0, 0], moment_in[0, 1])

    def finish(trio):
        down, gate, up = trio
        return jnp.stack([gate, up])[None], down[None]

    def synchronize():
        results = []
        for fresh, outer, moment in zip(new, outers, moments):
            mean = outer - total(fresh) / replicas
            next_moment = MOMENTUM * moment + mean
            next_outer = outer - OUTER_LR * (mean + MOMENTUM * next_moment)
            results.append((next_outer.astype(jnp.bfloat16), next_outer, next_moment))
        return tuple(finish(trio) for trio in zip(*results))

    def keep():
        return finish(new), (outer_in, outer_down), (moment_in, moment_down)

    (news, outer_results, moment_results) = lax.cond(chosen, synchronize, keep)
    return (news[0][None], news[1][None]) + outer_results + moment_results


def solution(mesh):
    return jax.shard_map(
        shards,
        mesh=mesh,
        in_specs=(
            P("rep", None, "tp"),
            P("section", None),
            P("rep", "section", None, None, "tp"),
            P("rep", "section", "tp", None),
            P("section", None, None, "tp"),
            P("section", "tp", None),
            P("section", None, None, "tp"),
            P("section", "tp", None),
            P("rep", None, "tp", None),
            P(),
        ),
        out_specs=(
            P("rep", "section", None, None, "tp"),
            P("rep", "section", "tp", None),
            P("section", None, None, "tp"),
            P("section", "tp", None),
            P("section", None, None, "tp"),
            P("section", "tp", None),
        ),
        check_vma=False,
    )
```

```python
import functools

import jax
import jax.numpy as jnp
from jax import lax
from jax.experimental import pallas as pl
from jax.experimental.pallas import tpu as pltpu
from jax.sharding import PartitionSpec as P

EPS = 1e-05
INNER_LR = 0.001
OUTER_LR = 0.7
MOMENTUM = 0.9
DELAY = 2
MESH = pl.DeviceIdType.MESH
NT = (((1,), (1,)), ((), ()))


def scale_rows(values):
    return lax.rsqrt(jnp.mean(values * values, axis=-1, keepdims=True) + EPS)


def dot(left, right):
    return jnp.dot(left, right, preferred_element_type=jnp.float32)


def dot_nt(left, right):
    return lax.dot_general(left, right, NT, preferred_element_type=jnp.float32)


def relay(
    sections,
    peers,
    looked,
    seeds,
    pair,
    down,
    normed_out,
    hidden_out,
    d_gate_out,
    d_up_out,
    grad_out,
    x_full,
    grad_full,
    part,
    back_part,
    inbox,
    back_inbox,
    rows_out,
    back_rows_out,
    gate_store,
    up_store,
    x_recv,
    grad_recv,
    part_recv,
    back_recv,
    x_send,
    grad_send,
    part_send,
    back_send,
    x_first,
    grad_first,
    rows_in,
    looked_box,
    looked_recv,
    looked_send,
):
    section = lax.axis_index("section")
    me = lax.axis_index("tp")
    batches, own, _ = looked.shape
    first = section == 0
    final = section == sections - 1
    later = section < sections - 1
    after = section > 0

    def rows_of(index):
        return pl.ds(pl.multiple_of(index * own, own), own)

    mine = rows_of(me)

    def wait(ref, sem):
        pltpu.make_async_copy(ref, ref, sem).wait()

    def send(source, target, send_sem, recv_sem, device):
        pltpu.make_async_remote_copy(
            src_ref=source,
            dst_ref=target,
            send_sem=send_sem,
            recv_sem=recv_sem,
            device_id=device,
            device_id_type=MESH,
        ).start()

    def around(offset):
        return lax.rem(me + offset, peers)

    barrier = pltpu.get_barrier_semaphore()
    for offset in range(1, peers):
        pl.semaphore_signal(
            barrier, inc=1, device_id={"tp": around(offset)}, device_id_type=MESH
        )

    @pl.when(later)
    def _():
        for offset in range(peers):
            pl.semaphore_signal(
                barrier,
                inc=1,
                device_id={"section": section + 1, "tp": around(offset)},
                device_id_type=MESH,
            )

    @pl.when(after)
    def _():
        for offset in range(peers):
            pl.semaphore_signal(
                barrier,
                inc=1,
                device_id={"section": section - 1, "tp": around(offset)},
                device_id_type=MESH,
            )

    @pl.when(first)
    def _():
        for other in range(2, sections):
            pl.semaphore_signal(
                barrier, inc=1, device_id={"section": other}, device_id_type=MESH
            )
        pl.semaphore_wait(barrier, 2 * peers - 1 + max(sections - 2, 0))

    @pl.when(section == 1)
    def _():
        pl.semaphore_wait(barrier, (3 if sections > 2 else 2) * peers - 1)

    @pl.when(section >= 2)
    def _():
        pl.semaphore_signal(barrier, inc=1, device_id={"section": 0}, device_id_type=MESH)

    @pl.when((section >= 2) & later)
    def _():
        pl.semaphore_wait(barrier, 3 * peers)

    @pl.when((section >= 2) & final)
    def _():
        pl.semaphore_wait(barrier, 2 * peers)

    def spread(micro, rows, full, send_sem, recv_sem):
        for offset in range(1, peers):
            send(
                rows.at[micro],
                full.at[micro, mine],
                send_sem.at[micro],
                recv_sem.at[micro],
                {"tp": around(offset)},
            )
        full[micro, mine, :] = rows[micro]

    def feed(micro):
        total = looked[micro]
        for slot in range(sections - 1):
            wait(looked_box.at[slot, micro], looked_recv.at[slot, micro])
            total += looked_box[slot, micro]
        rows_in[micro] = total
        spread(micro, rows_in, x_full, x_first, x_recv)

    @pl.when(after)
    def _():
        def give(micro, carry):
            send(
                looked.at[micro],
                looked_box.at[section - 1, micro],
                looked_send.at[micro],
                looked_recv.at[section - 1, micro],
                {"section": 0},
            )
            return carry

        lax.fori_loop(0, batches, give, 0)

    @pl.when(final)
    def _():
        def give(micro, carry):
            spread(micro, seeds, grad_full, grad_first, grad_recv)
            return carry

        lax.fori_loop(0, batches, give, 0)

    @pl.when(first)
    def _():
        for micro in range(min(2, batches)):
            feed(micro)

    def arrive(micro, full, recv_sem, alone):
        @pl.when(alone)
        def _():
            wait(full.at[micro, pl.ds(0, (peers - 1) * own)], recv_sem.at[micro])

        @pl.when(jnp.logical_not(alone))
        def _():
            wait(full.at[micro], recv_sem.at[micro])

    def scatter(micro, source, box, send_sem, recv_sem):
        for offset in range(1, peers):
            send(
                source.at[micro, rows_of(around(offset))],
                box.at[micro, offset - 1],
                send_sem.at[micro],
                recv_sem.at[micro],
                {"tp": around(offset)},
            )

    def collect(micro, source, box, recv_sem):
        wait(box.at[micro], recv_sem.at[micro])
        total = source[micro, mine, :].astype(jnp.float32)
        for slot in range(peers - 1):
            total += box[micro, slot].astype(jnp.float32)
        return total

    def pass_along(micro, rows, full, send_sem, recv_sem, step):
        for offset in range(peers):
            send(
                rows.at[micro],
                full.at[micro, mine],
                send_sem.at[micro],
                recv_sem.at[micro],
                {"section": section + step, "tp": around(offset)},
            )

    def forward(micro):
        arrive(micro, x_full, x_recv, first)
        xf = x_full[micro].astype(jnp.float32)
        normed = (xf * scale_rows(xf)).astype(jnp.bfloat16)
        normed_out[micro] = normed
        gate = dot(normed, pair[0])
        upper = dot(normed, pair[1])
        gate_store[micro] = gate
        up_store[micro] = upper
        hidden = (gate * jax.nn.sigmoid(gate) * upper).astype(jnp.bfloat16)
        hidden_out[micro] = hidden

        @pl.when(later)
        def _():
            part[micro] = dot(hidden, down[...]).astype(jnp.bfloat16)
            scatter(micro, part, inbox, part_send, part_recv)

    def forward_end(micro):
        total = collect(micro, part, inbox, part_recv)
        xf = x_full[micro, mine, :].astype(jnp.float32)
        rows_out[micro] = (xf + total).astype(jnp.bfloat16)
        pass_along(micro, rows_out, x_full, x_send, x_recv, 1)

    def backward(micro):
        arrive(micro, grad_full, grad_recv, final)
        grad = grad_full[micro]
        grad_out[micro] = grad
        d_hidden = dot_nt(grad, down[...])
        gate = gate_store[micro]
        sig = jax.nn.sigmoid(gate)
        d_gate = (d_hidden * up_store[micro] * sig * (1.0 + gate * (1.0 - sig))).astype(
            jnp.bfloat16
        )
        d_up = (d_hidden * (gate * sig)).astype(jnp.bfloat16)
        d_gate_out[micro] = d_gate
        d_up_out[micro] = d_up

        @pl.when(after)
        def _():
            back_part[micro] = (dot_nt(d_gate, pair[0]) + dot_nt(d_up, pair[1])).astype(
                jnp.bfloat16
            )
            scatter(micro, back_part, back_inbox, back_send, back_recv)

    def backward_end(micro):
        d_norm = collect(micro, back_part, back_inbox, back_recv)
        xf = x_full[micro, mine, :].astype(jnp.float32)
        rinv = scale_rows(xf)
        d_x = (
            grad_full[micro, mine, :].astype(jnp.float32)
            + rinv * d_norm
            - xf * (rinv * rinv * rinv) * jnp.mean(d_norm * xf, axis=-1, keepdims=True)
        )
        back_rows_out[micro] = d_x.astype(jnp.bfloat16)
        pass_along(micro, back_rows_out, grad_full, grad_send, grad_recv, -1)

    delay = DELAY * (sections - 1 - section)

    def step(tick, carry):
        @pl.when(first & (tick + 2 < batches))
        def _():
            feed(tick + 2)

        micro = tick - delay
        ahead = tick < batches
        behind = (micro >= 0) & (micro < batches)

        @pl.when(ahead)
        def _():
            forward(tick)

        @pl.when(later & ahead)
        def _():
            forward_end(tick)

        @pl.when(behind)
        def _():
            backward(micro)

        @pl.when(after & behind)
        def _():
            backward_end(micro)

        return carry

    lax.fori_loop(0, batches + DELAY * (sections - 1) + 1, step, 0)

    def drain(micro, carry):
        some = pl.ds(0, (peers - 1) * own)

        @pl.when(first)
        def _():
            wait(x_full.at[micro, some], x_first.at[micro])

        @pl.when(final)
        def _():
            wait(grad_full.at[micro, some], grad_first.at[micro])

        @pl.when(later)
        def _():
            wait(part.at[micro, some], part_send.at[micro])
            wait(x_full.at[micro], x_send.at[micro])

        @pl.when(after)
        def _():
            wait(looked.at[micro], looked_send.at[micro])
            wait(back_part.at[micro, some], back_send.at[micro])
            wait(grad_full.at[micro], grad_send.at[micro])

        return carry

    lax.fori_loop(0, batches, drain, 0)


def run_relay(x0, seeds, pair, down):
    sections, peers = lax.axis_size("section"), lax.axis_size("tp")
    batches, own, width = x0.shape
    hidden = down.shape[0]
    rows = own * peers

    def of(*shape, kind=jnp.bfloat16):
        return pltpu.VMEM((batches,) + shape, kind)

    def out(columns):
        return jax.ShapeDtypeStruct((batches, rows, columns), jnp.bfloat16)

    vmem = pl.BlockSpec(memory_space=pltpu.VMEM)
    flops = 2 * batches * rows * width * hidden * 6
    return pl.pallas_call(
        functools.partial(relay, sections, peers),
        out_shape=(out(width), out(hidden), out(hidden), out(hidden), out(width)),
        in_specs=[vmem] * 4,
        out_specs=(vmem,) * 5,
        scratch_shapes=[
            of(rows, width),
            of(rows, width),
            of(rows, width),
            of(rows, width),
            of(peers - 1, own, width),
            of(peers - 1, own, width),
            of(own, width),
            of(own, width),
            of(rows, hidden, kind=jnp.float32),
            of(rows, hidden, kind=jnp.float32),
        ]
        + [pltpu.SemaphoreType.DMA((batches,))] * 10
        + [
            of(own, width),
            pltpu.VMEM((sections - 1, batches, own, width), jnp.bfloat16),
            pltpu.SemaphoreType.DMA((sections - 1, batches)),
            pltpu.SemaphoreType.DMA((batches,)),
        ],
        compiler_params=pltpu.CompilerParams(
            collective_id=0, has_side_effects=True, vmem_limit_bytes=60 * 1024 * 1024
        ),
        cost_estimate=pl.CostEstimate(
            flops=flops, bytes_accessed=32 * 1024 * 1024, transcendentals=0
        ),
    )(x0, seeds, pair, down)


def shards(
    token_ids,
    embed,
    w_in,
    w_down,
    outer_in,
    outer_down,
    moment_in,
    moment_down,
    cotangent,
    fragment,
):
    sections = lax.axis_size("section")
    section = lax.axis_index("section")
    replicas = lax.axis_size("rep")
    ids = token_ids[0]
    batches, own_rows = ids.shape
    vocab_part, width = embed.shape
    local_ids = ids - section * vocab_part
    inside = (local_ids >= 0) & (local_ids < vocab_part)
    looked = jnp.take(embed, jnp.clip(local_ids, 0, vocab_part - 1), axis=0)
    start_rows = jnp.where(inside[:, :, None], looked, jnp.zeros_like(looked))
    pairs = w_in[0, 0]
    downs = w_down[0, 0]
    normed, hidden, d_gate, d_up, grad = run_relay(start_rows, cotangent[0], pairs, downs)

    def weight_grad(left, right):
        return jnp.einsum("bti,btj->ij", left, right, preferred_element_type=jnp.float32)

    def other(values):
        return lax.ppermute(
            values, "rep", [(source, (source + 1) % replicas) for source in range(replicas)]
        )

    def total(values):
        summed = values.astype(jnp.float32)
        passing = values
        for _ in range(replicas - 1):
            passing = other(passing)
            summed = summed + passing.astype(jnp.float32)
        return summed

    def inner(weights, grads):
        return (weights.astype(jnp.float32) - INNER_LR * grads).astype(jnp.bfloat16)

    flag = lax.dynamic_index_in_dim(fragment, section, 0, keepdims=False)
    chosen = flag == 1

    new = (
        inner(downs, weight_grad(hidden, grad)),
        inner(pairs[0], weight_grad(normed, d_gate)),
        inner(pairs[1], weight_grad(normed, d_up)),
    )
    outers = (outer_down[0], outer_in[0, 0], outer_in[0, 1])
    moments = (moment_down[0], moment_in[0, 0], moment_in[0, 1])

    def finish(trio):
        down, gate, up = trio
        return jnp.stack([gate, up])[None], down[None]

    def synchronize():
        results = []
        for fresh, outer, moment in zip(new, outers, moments):
            mean = outer - total(fresh) / replicas
            next_moment = MOMENTUM * moment + mean
            next_outer = outer - OUTER_LR * (mean + MOMENTUM * next_moment)
            results.append((next_outer.astype(jnp.bfloat16), next_outer, next_moment))
        return tuple(finish(trio) for trio in zip(*results))

    def keep():
        return finish(new), (outer_in, outer_down), (moment_in, moment_down)

    (news, outer_results, moment_results) = lax.cond(chosen, synchronize, keep)
    return (news[0][None], news[1][None]) + outer_results + moment_results


def solution(mesh):
    return jax.shard_map(
        shards,
        mesh=mesh,
        in_specs=(
            P("rep", None, "tp"),
            P("section", None),
            P("rep", "section", None, None, "tp"),
            P("rep", "section", "tp", None),
            P("section", None, None, "tp"),
            P("section", "tp", None),
            P("section", None, None, "tp"),
            P("section", "tp", None),
            P("rep", None, "tp", None),
            P(),
        ),
        out_specs=(
            P("rep", "section", None, None, "tp"),
            P("rep", "section", "tp", None),
            P("section", None, None, "tp"),
            P("section", "tp", None),
            P("section", None, None, "tp"),
            P("section", "tp", None),
        ),
        check_vma=False,
    )
```
